32 devices in a mesh: gx: 4 (over y, x), gy: 8 (over z, core).
Axes of the slice: x: 2, y: 2, z: 4, core: 2. Of those that a mesh axis runs over, the one named last changes fastest.
Arguments:
- positions: float32 [3, 262144], P(None, ('gx', 'gy')), may hold values from -6 to 6
- velocities: float32 [3, 262144], P(None, ('gx', 'gy')), may hold values from -4 to 4
- masses: float32 [262144], P(('gx', 'gy')), may hold values from 0.005 to 0.05
- long_kick: float32 [3, 262144], P(None, ('gx', 'gy')), may hold values from -3 to 3
- leaf_lists: int32 [8, 2048], P(None, ('gx', 'gy')), may hold values from 0 to 135, as said below
- ghost_ids: int32 [256], P(('gx', 'gy')), may hold values from 0 to 63, as said below
- leaf_counts: int32 [32], P(('gx', 'gy')), may hold values from 1 to 64, as said below
Outputs:
- new_positions: float32 [3, 262144], P(None, ('gx', 'gy'))
- new_velocities: float32 [3, 262144], P(None, ('gx', 'gy'))
The draws below stay inside these ranges and needn't reach their ends.
Inputs may be any that keep to these rules, and one draw needn't show every extreme that they name: leaf_counts of a domain is at least 1; the counts of domains (i, j) and (i, j + 4) for j below 4 sum to at most 80, and some pair reaches it with one count equal to 64. `leaf_lists`: every entry below 64 is below the count of its domain; entries from 64 on name pool ghost leaves. `ghost_ids`: each id is below the count of its domain; ids may repeat.
All inputs are finite; a program needn't handle non-finite values.
Results may differ from the reference program's by a relative error of at most 0.00011.
Values sent between devices are 32-bit elements; how exact they have to be, the bound alone decides.
A program may use at most 64 MiB of HBM per device.

```python
import math
import jax
import jax.numpy as jnp
from jax import lax

LEAF = 128
NEIGHBOURS = 8
LEAVES = 64
GHOSTS = 8
SUBCYCLES = 4
BAL = 40
SLABS = 4
COLUMNS = 8
DOMAINS = 32
PARTICLES = 262144


def pair_counts(key):
    base = jax.random.fold_in(key, 7)
    first_key, second_key = jax.random.split(base)
    half = COLUMNS // 2
    totals = jax.random.randint(first_key, (SLABS, half), 4, 2 * BAL + 1)
    totals = totals.at[0, 0].set(2 * BAL)
    lowest = jnp.maximum(1, totals - LEAVES)
    highest = jnp.minimum(LEAVES, totals - 1)
    first = jax.random.randint(second_key, (SLABS, half), lowest, highest + 1)
    first = first.at[0, 0].set(LEAVES)
    second = totals - first
    return jnp.concatenate([first, second], axis=1).reshape(-1).astype(jnp.int32)


def draw_leaf_counts(key, part):
    return pair_counts(key)


def draw_leaf_lists(key, part):
    counts = pair_counts(key)
    per_leaf = jnp.repeat(counts, LEAVES, total_repeat_length=DOMAINS * LEAVES)
    base = jax.random.fold_in(key, 11)
    own_key, ghost_key, pick_key = jax.random.split(base, 3)
    shape = (NEIGHBOURS, DOMAINS * LEAVES)
    own_pick = jax.random.randint(own_key, shape, 0, jnp.broadcast_to(per_leaf[None, :], shape))
    ghost_pick = LEAVES + jax.random.randint(ghost_key, shape, 0, 9 * GHOSTS)
    which = jax.random.randint(pick_key, shape, 0, 2)
    return jnp.where(which == 1, ghost_pick, own_pick).astype(jnp.int32)


def draw_ghost_ids(key, part):
    counts = pair_counts(key)
    per_ghost = jnp.repeat(counts, GHOSTS, total_repeat_length=DOMAINS * GHOSTS)
    base = jax.random.fold_in(key, 13)
    return jax.random.randint(base, (DOMAINS * GHOSTS,), 0, per_ghost).astype(jnp.int32)


def levels(key, shape, cuts, low, largest):
    def one(dim, blocks):
        steps = jax.random.uniform(jax.random.fold_in(jax.random.fold_in(key, 6), dim), (blocks,), jnp.float32, low / len(cuts), largest / len(cuts))
        return jnp.repeat(jnp.exp(steps), shape[dim] // blocks).reshape((-1,) + (1,) * (len(shape) - dim - 1))

    gain = one(*cuts[0])
    for cut in cuts[1:]:
        gain = gain * one(*cut)
    return gain


def scatter_about(rng, extent, deviation, limit, cuts=(), held_as=jnp.bfloat16):
    level = levels(rng, extent, cuts, -0.22, 0.18) if cuts else 1.0
    result = jax.random.normal(rng, extent, jnp.float32) * deviation * level
    return jnp.minimum(jnp.maximum(result, -limit), limit).astype(held_as)


def setup_inputs(seed: int = 0) -> dict:
    key_list = jax.random.split(jax.random.key(seed), 8)
    return {
        "positions": scatter_about(key_list[0], (3, PARTICLES), 1.0, 6.0, ((1, 32),), jnp.float32),
        "velocities": scatter_about(key_list[1], (3, PARTICLES), 0.5, 4.0, ((1, 32),), jnp.float32),
        "masses": jnp.clip(jnp.exp(math.log(0.05) - 2.3025851 * jax.random.uniform(key_list[2], (PARTICLES,), jnp.float32) ** levels(key_list[2], (PARTICLES,), ((0, 32),), -0.2, 0.2)), 0.005, 0.05),
        "long_kick": scatter_about(key_list[3], (3, PARTICLES), 0.3, 3.0, ((1, 32),), jnp.float32),
        "leaf_lists": draw_leaf_lists(jax.random.fold_in(key_list[7], 71), 0),
        "ghost_ids": draw_ghost_ids(jax.random.fold_in(key_list[7], 71), 0),
        "leaf_counts": draw_leaf_counts(jax.random.fold_in(key_list[7], 71), 0),
    }


soften_sq = 0.04
cutoff_sq = 9.0
time_step = 0.5

def pair_accel(targets, sources):
    offsets = sources[:3, :, None, :] - targets[:, :, :, None]
    distance = lax.optimization_barrier(jnp.sum(offsets * offsets, axis=0))
    tapers = jnp.square(jnp.maximum(1.0 - distance / cutoff_sq, 0.0))
    inverse = lax.rsqrt(distance + soften_sq)
    weight = sources[3][:, None, :] * tapers * inverse * inverse * inverse
    return lax.optimization_barrier(jnp.sum(offsets * weight[None], axis=3))

def accumulate(targets, operands):

    def add_tile(index, summed):
        sources = lax.dynamic_index_in_dim(operands, index, 1, keepdims=False)
        return summed + pair_accel(targets, sources)
    return lax.fori_loop(0, operands.shape[1], add_tile, jnp.zeros(targets.shape, targets.dtype))

def gather_pool(pool_rows, list_rows):
    return jnp.take(pool_rows, list_rows, axis=1)

def reference(positions, velocities, masses, long_kick, leaf_lists, ghost_ids, leaf_counts):
    places = jnp.moveaxis(positions.reshape(3, SLABS, COLUMNS, LEAVES, LEAF), 0, 2)
    speeds = jnp.moveaxis(velocities.reshape(3, SLABS, COLUMNS, LEAVES, LEAF), 0, 2)
    kicks = jnp.moveaxis(long_kick.reshape(3, SLABS, COLUMNS, LEAVES, LEAF), 0, 2)
    mass_rows = masses.reshape(SLABS, COLUMNS, 1, LEAVES, LEAF)
    lists = jnp.moveaxis(leaf_lists.reshape(NEIGHBOURS, SLABS, COLUMNS, LEAVES), 0, 2)
    ghosts = ghost_ids.reshape(SLABS, COLUMNS, 1, GHOSTS, 1)
    ghosts = jnp.broadcast_to(ghosts, (SLABS, COLUMNS, 4, GHOSTS, LEAF))
    counts = leaf_counts.reshape(SLABS, COLUMNS, 1, 1, 1)
    live = jnp.arange(LEAVES).astype(jnp.int32)[None, None, None, :, None] < counts
    for subcycle in range(SUBCYCLES):
        own_rows = jnp.concatenate([places, mass_rows], axis=2)
        chosen = jnp.take_along_axis(own_rows, ghosts, axis=3)
        parts = [own_rows]
        for shift_x in (-1, 0, 1):
            for shift_y in (-1, 0, 1):
                parts.append(jnp.roll(jnp.roll(chosen, -shift_x, axis=0), -shift_y, axis=1))
        pool = jnp.concatenate(parts, axis=3)
        operands = jax.vmap(jax.vmap(gather_pool))(pool, lists)

        def slab_accel(items):
            return jax.vmap(accumulate)(items[0], items[1])
        accel = lax.map(slab_accel, (places, operands))
        speeds = jnp.where(live, speeds + time_step * (accel + kicks), speeds)
        places = jnp.where(live, places + time_step * speeds, places)
    new_positions = jnp.moveaxis(places, 2, 0).reshape(3, -1)
    new_velocities = jnp.moveaxis(speeds, 2, 0).reshape(3, -1)
    return (new_positions, new_velocities)
```

```python
import functools

import jax
import jax.numpy as jnp
from jax import lax
from jax.experimental import pallas as pl
from jax.experimental.pallas import tpu as pltpu
from jax.sharding import PartitionSpec as P

SUBCYCLES = 4

soften_sq = 0.04
cutoff_sq = 9.0
time_step = 0.5

MESH = pl.DeviceIdType.MESH
PAIR_ROWS = 32
SUM_ROWS = 16
WAYS = [(a, b) for a in (-1, 0, 1) for b in (-1, 0, 1)]
BESIDE = [way for way in WAYS if way != (0, 0)]
UNROLL = 16
GROUP = 4
ROUND_UP = 1.0 + 2.0**-22


def thirds(value):
    first = value.astype(jnp.bfloat16).astype(jnp.float32)
    rest = value - first
    second = rest.astype(jnp.bfloat16).astype(jnp.float32)
    return first, second, rest - second


def slot_of(a, b):
    return (a + 1) * 3 + b + 1


def kernel(
    sizes, p_in, v_in, mass, kick, live_in, lists, ghosts, p, v,
    wide, heavy, pool, carry, targets, narrow, sums, ghost_sums, ghost_v, ghost_kick, sent, got,
    send_sem, recv_sem,
):
    nx, ny = sizes
    leaves, lanes = mass.shape
    entries = lists.shape[0]
    lent = ghosts.shape[0]
    slots = wide.shape[0] // PAIR_ROWS
    me_x, me_y = lax.axis_index("gx"), lax.axis_index("gy")

    def device(a, b):
        return (lax.rem(me_x + (a + nx), nx), lax.rem(me_y + (b + ny), ny))

    barrier = pltpu.get_barrier_semaphore()
    for a, b in BESIDE:
        pl.semaphore_signal(barrier, inc=1, device_id=device(a, b), device_id_type=MESH)

    p[...] = p_in[...]
    v[...] = v_in[...]
    for g in range(lent):
        leaf = ghosts[g]
        for c in range(3):
            sent[0, c, g] = p_in[c, leaf]
            ghost_v[c, g] = v_in[c, leaf]
            ghost_kick[c, g] = kick[c, leaf]
        row = mass[leaf]
        for k in range(SUBCYCLES):
            sent[k, 3, g] = row

    def copies(k):
        made = []
        for a, b in BESIDE:
            made.append(
                pltpu.make_async_remote_copy(
                    src_ref=sent.at[k],
                    dst_ref=got.at[k, slot_of(-a, -b)],
                    send_sem=send_sem.at[k, slot_of(a, b)],
                    recv_sem=recv_sem.at[k, slot_of(-a, -b)],
                    device_id=device(a, b),
                    device_id_type=MESH,
                )
            )
        return made

    flying = []
    pl.semaphore_wait(barrier, len(BESIDE))
    flying.append(copies(0))
    for copy in flying[0]:
        copy.start()

    def put(ref, height, base, total, row, value):
        ref[pl.ds(base * height + row, total, stride=height), :] = value

    ones = jnp.ones((slots, lanes), jnp.float32)
    zeros = jnp.zeros((slots, lanes), jnp.float32)
    for row in range(18, 21):
        put(targets, PAIR_ROWS, 0, leaves, row, ones[:leaves])
    for row in range(21, 24):
        put(wide, PAIR_ROWS, 0, slots, row, ones)
    for row in range(24, PAIR_ROWS):
        put(wide, PAIR_ROWS, 0, slots, row, zeros)
        put(targets, PAIR_ROWS, 0, leaves, row, zeros[:leaves])
    for row in range(12, SUM_ROWS):
        put(heavy, SUM_ROWS, 0, slots, row, zeros)

    def lay_out(base, total, place, weight):
        norm = None
        splits = []
        for c in range(3):
            scaled = place[c] * (cutoff_sq**-0.5)
            square = scaled * scaled
            norm = square if norm is None else norm + square
            one, two, three = thirds(scaled)
            splits.append((one, two, three))
            for row, value in enumerate((one, two, one, three, one, two)):
                put(wide, PAIR_ROWS, base, total, c * 6 + row, value)
        norm = norm * ROUND_UP
        for row, value in enumerate(thirds(-norm)):
            put(wide, PAIR_ROWS, base, total, 18 + row, value)
        scaled_weight = weight * (cutoff_sq**-1.5)
        moments = [scaled_weight] + [scaled_weight * place[c] for c in range(3)]
        for c, moment in enumerate(moments):
            for row, value in enumerate(thirds(moment)):
                put(heavy, SUM_ROWS, base, total, c * 3 + row, value)
        return splits, norm

    blank = jnp.zeros((lanes, lanes), jnp.bfloat16)

    def leaf_sums(leaf, out, where):
        near = [lists[e, leaf] for e in range(entries)]
        target = jnp.concatenate([narrow[leaf]] * GROUP, axis=0)
        pair = jnp.concatenate(
            [
                jnp.concatenate([target, blank], axis=1),
                jnp.concatenate([blank, target], axis=1),
            ],
            axis=0,
        )
        total = None
        for j in range(0, entries, 2):
            source = jnp.concatenate([pool[near[j]], pool[near[j + 1]]], axis=1)
            inside = jnp.dot(source, pair, preferred_element_type=jnp.float32)
            rows = []
            for half in range(2):
                close = inside[:, half * lanes : (half + 1) * lanes]
                inverse = lax.rsqrt((1.0 + soften_sq / cutoff_sq) - close)
                taper = jnp.maximum(close * inverse, 0.0)
                weight = taper * taper * inverse
                high = weight.astype(jnp.bfloat16)
                low = (weight - high.astype(jnp.float32)).astype(jnp.bfloat16)
                rows.append(jnp.concatenate([high, low], axis=1))
            moments = jnp.concatenate([carry[near[j]], carry[near[j + 1]]], axis=1)
            part = jnp.dot(
                moments, jnp.concatenate(rows, axis=0), preferred_element_type=jnp.float32
            )
            total = part if total is None else total + part
        out[pl.ds(pl.multiple_of(where * SUM_ROWS, SUM_ROWS), SUM_ROWS), :] = (
            total[:, :lanes] + total[:, lanes:]
        )

    def gathered(ref, total):
        parts = []
        for c in range(4):
            rows = [ref[pl.ds(c * 3 + r, total, stride=SUM_ROWS), :] for r in range(3)]
            parts.append(rows[0] + (rows[1] + rows[2]))
        return parts

    live = time_step * live_in[...]

    for k in range(SUBCYCLES):
        splits, norm = lay_out(0, leaves, [p[c] for c in range(3)], mass[...])
        for c in range(3):
            one, two, three = [2.0 * part for part in splits[c]]
            for row, value in enumerate((one, one, two, one, three, two)):
                put(targets, PAIR_ROWS, 0, leaves, c * 6 + row, value)
        for row, value in enumerate(thirds(1.0 - norm)):
            put(targets, PAIR_ROWS, 0, leaves, 21 + row, value)
        lay_out(
            leaves + slot_of(0, 0) * lent, lent, [sent[k, c] for c in range(3)], sent[k, 3]
        )
        for copy in flying[k]:
            copy.wait_recv()
        for a, b in BESIDE:
            at = slot_of(a, b)
            lay_out(leaves + at * lent, lent, [got[k, at, c] for c in range(3)], got[k, at, 3])

        spot = lax.broadcasted_iota(jnp.int32, (lanes, lanes), 1) // PAIR_ROWS
        keep = [(spot == g).astype(jnp.float32).astype(jnp.bfloat16) for g in range(GROUP)]

        def turn(i, _):
            rows = pl.ds(pl.multiple_of(i * lanes, lanes), lanes)
            block = wide[rows, :].T.astype(jnp.bfloat16)
            for g in range(GROUP):
                pool[i * GROUP + g] = block * keep[g]
            rows = pl.ds(pl.multiple_of(i * (GROUP * SUM_ROWS), GROUP * SUM_ROWS), GROUP * SUM_ROWS)
            tiles = heavy[rows, :].astype(jnp.bfloat16).reshape(GROUP, SUM_ROWS, lanes)
            carry[pl.ds(i * GROUP, GROUP)] = tiles
            return _

        lax.fori_loop(0, slots // GROUP, turn, 0)

        def shrink(i, _):
            rows = pl.ds(pl.multiple_of(i * lanes, lanes), lanes)
            tiles = targets[rows, :].astype(jnp.bfloat16).reshape(GROUP, PAIR_ROWS, lanes)
            narrow[pl.ds(i * GROUP, GROUP)] = tiles
            return _

        lax.fori_loop(0, leaves // GROUP, shrink, 0)

        if k + 1 < SUBCYCLES:

            for g in range(lent):
                leaf_sums(ghosts[g], ghost_sums, g)
            total, *moments = gathered(ghost_sums, lent)
            for c in range(3):
                place = sent[k, c]
                accel = moments[c] - total * place
                speed = ghost_v[c] + time_step * (accel + ghost_kick[c])
                ghost_v[c] = speed
                sent[k + 1, c] = place + time_step * speed
            flying.append(copies(k + 1))
            for copy in flying[k + 1]:
                copy.start()

        def pull(i, _):
            for u in range(UNROLL):
                leaf = i * UNROLL + u
                leaf_sums(leaf, sums, leaf)
            return _

        lax.fori_loop(0, leaves // UNROLL, pull, 0)
        total, *moments = gathered(sums, leaves)
        for c in range(3):
            place, speed = p[c], v[c]
            accel = moments[c] - total * place
            faster = speed + live * (accel + kick[c])
            v[c] = faster
            p[c] = place + live * faster

    for made in flying:
        for copy in made:
            copy.wait_send()


def solution(mesh):
    sizes = (mesh.shape["gx"], mesh.shape["gy"])

    def body(positions, velocities, masses, long_kick, leaf_lists, ghost_ids, leaf_counts):
        leaves = leaf_lists.shape[1]
        lanes = masses.shape[0] // leaves
        lent = ghost_ids.shape[0]
        slots = leaves + len(WAYS) * lent
        state = jax.ShapeDtypeStruct((3, leaves, lanes), jnp.float32)
        live = (jnp.arange(leaves)[:, None] < leaf_counts).astype(jnp.float32)
        live = jnp.broadcast_to(live, (leaves, lanes))
        vmem = pl.BlockSpec(memory_space=pltpu.VMEM)
        smem = pl.BlockSpec(memory_space=pltpu.SMEM)
        f32 = jnp.float32
        places, speeds = pl.pallas_call(
            functools.partial(kernel, sizes),
            out_shape=(state, state),
            in_specs=[vmem] * 5 + [smem] * 2,
            out_specs=(vmem, vmem),
            scratch_shapes=[
                pltpu.VMEM((slots * PAIR_ROWS, lanes), f32),
                pltpu.VMEM((slots * SUM_ROWS, lanes), f32),
                pltpu.VMEM((slots, lanes, lanes), jnp.bfloat16),
                pltpu.VMEM((slots, SUM_ROWS, lanes), jnp.bfloat16),
                pltpu.VMEM((leaves * PAIR_ROWS, lanes), f32),
                pltpu.VMEM((leaves, PAIR_ROWS, lanes), jnp.bfloat16),
                pltpu.VMEM((leaves * SUM_ROWS, lanes), f32),
                pltpu.VMEM((lent * SUM_ROWS, lanes), f32),
                pltpu.VMEM((3, lent, lanes), f32),
                pltpu.VMEM((3, lent, lanes), f32),
                pltpu.VMEM((SUBCYCLES, 4, lent, lanes), f32),
                pltpu.VMEM((SUBCYCLES, len(WAYS), 4, lent, lanes), f32),
                pltpu.SemaphoreType.DMA((SUBCYCLES, len(WAYS))),
                pltpu.SemaphoreType.DMA((SUBCYCLES, len(WAYS))),
            ],
            compiler_params=pltpu.CompilerParams(collective_id=0, has_side_effects=True),
        )(
            positions.reshape(3, leaves, lanes),
            velocities.reshape(3, leaves, lanes),
            masses.reshape(leaves, lanes),
            long_kick.reshape(3, leaves, lanes),
            live,
            leaf_lists,
            ghost_ids,
        )
        return places.reshape(3, -1), speeds.reshape(3, -1)

    return jax.shard_map(
        body,
        mesh=mesh,
        in_specs=(
            P(None, ("gx", "gy")),
            P(None, ("gx", "gy")),
            P(("gx", "gy")),
            P(None, ("gx", "gy")),
            P(None, ("gx", "gy")),
            P(("gx", "gy")),
            P(("gx", "gy")),
        ),
        out_specs=(P(None, ("gx", "gy")), P(None, ("gx", "gy"))),
        check_vma=False,
    )
```

```python
import functools

import jax
import jax.numpy as jnp
from jax import lax
from jax.experimental import pallas as pl
from jax.experimental.pallas import tpu as pltpu
from jax.sharding import PartitionSpec as P

SUBCYCLES = 4

soften_sq = 0.04
cutoff_sq = 9.0
time_step = 0.5

MESH = pl.DeviceIdType.MESH
COMPS = 4
PAIR = 2 * COMPS
GROUP = 4
SUM_ROWS = 16
TARGET_ROWS = 8 * PAIR
UNROLL = 16
ROUND_UP = 1.0 + 2.0**-22
WAYS = [(a, b) for a in (-1, 0, 1) for b in (-1, 0, 1)]
BESIDE = [way for way in WAYS if way != (0, 0)]


def thirds(value):
    first = value.astype(jnp.bfloat16).astype(jnp.float32)
    rest = value - first
    second = rest.astype(jnp.bfloat16).astype(jnp.float32)
    return first, second, rest - second


def slot_of(a, b):
    return (a + 1) * 3 + b + 1


def kernel(
    sizes, p_in, v_in, mass, kick_in, lists, ghosts, count, p_out, v_out,
    p, v, kick, pool, carry, narrow, sums, ghost_sums, ghost_v, ghost_kick, sent, got,
    send_sem, recv_sem,
):
    nx, ny = sizes
    leaves, lanes = mass.shape
    entries = lists.shape[0]
    lent = ghosts.shape[0]
    me_x, me_y = lax.axis_index("gx"), lax.axis_index("gy")

    def device(a, b):
        return (lax.rem(me_x + (a + nx), nx), lax.rem(me_y + (b + ny), ny))

    barrier = pltpu.get_barrier_semaphore()
    for a, b in BESIDE:
        pl.semaphore_signal(barrier, inc=1, device_id=device(a, b), device_id_type=MESH)

    def rows_of(index, height):
        return pl.ds(pl.multiple_of(index * height, height), height)

    for g in range(lent):
        leaf = ghosts[g]
        at = pl.ds(g * COMPS, 3)
        last = pl.ds(g * COMPS + 3, 1)
        sent[0, at, :] = p_in[leaf]
        sent[0, last, :] = mass[pl.ds(leaf, 1), :]
        ghost_v[at, :] = v_in[leaf]
        ghost_v[last, :] = jnp.zeros((1, lanes), jnp.float32)
        ghost_kick[at, :] = kick_in[leaf]
        ghost_kick[last, :] = jnp.zeros((1, lanes), jnp.float32)

    def copies(k):
        made = []
        for a, b in BESIDE:
            made.append(
                pltpu.make_async_remote_copy(
                    src_ref=sent.at[k],
                    dst_ref=got.at[k, slot_of(-a, -b)],
                    send_sem=send_sem.at[k, slot_of(a, b)],
                    recv_sem=recv_sem.at[k, slot_of(-a, -b)],
                    device_id=device(a, b),
                    device_id_type=MESH,
                )
            )
        return made

    pl.semaphore_wait(barrier, len(BESIDE))
    for copy in copies(0):
        copy.start()

    for leaf in range(leaves):
        at = pl.ds(leaf * COMPS, 3)
        last = pl.ds(leaf * COMPS + 3, 1)
        p[at, :] = p_in[leaf]
        p[last, :] = mass[pl.ds(leaf, 1), :]
        v[at, :] = v_in[leaf]
        v[last, :] = jnp.zeros((1, lanes), jnp.float32)
        kick[at, :] = kick_in[leaf]
        kick[last, :] = jnp.zeros((1, lanes), jnp.float32)

    row = lax.broadcasted_iota(jnp.int32, (PAIR, lanes), 0)
    comp = row % COMPS
    former = row < COMPS
    weigh = comp == COMPS - 1
    zeros = jnp.zeros((PAIR, lanes), jnp.float32)
    ones = jnp.ones((PAIR, lanes), jnp.float32)
    lane = lax.broadcasted_iota(jnp.int32, (lanes, lanes), 1)
    quarter = lane // TARGET_ROWS * 2 + lane % PAIR // COMPS
    keep = [(quarter == g).astype(jnp.float32).astype(jnp.bfloat16) for g in range(GROUP)]
    blank = jnp.zeros((lanes, lanes), jnp.bfloat16)
    moving = jnp.where(weigh, 0.0, time_step)

    def roll(value, by):
        return pltpu.roll(value, by, 0)

    def all_rows(value):
        filled = jnp.where(comp == 0, roll(value, PAIR - 3), value)
        filled = jnp.where(comp == 1, roll(value, PAIR - 2), filled)
        return jnp.where(comp == 2, roll(value, PAIR - 1), filled)

    def halves(value):
        swapped = roll(value, COMPS)
        return jnp.where(former, value, swapped), jnp.where(former, swapped, value)

    def spread(place):
        scaled = place * (cutoff_sq**-0.5)
        square = scaled * scaled
        norm = (roll(square, 1) + (roll(square, 2) + roll(square, 3))) * ROUND_UP
        return thirds(jnp.where(weigh, -norm, scaled)), norm

    def lay_group(i, places, aims):
        tiles = []
        for j, place in enumerate(places):
            (one, two, three), norm = spread(place)
            tiles += [one, two, one, three, one, two, ones, zeros]
            heavy = all_rows(place) * (cutoff_sq**-1.5)
            moments = thirds(heavy * jnp.where(weigh, 1.0, place))
            firsts, seconds, rests = [halves(moment) for moment in moments]
            for h in range(2):
                top = jnp.where(former, firsts[h], seconds[h])
                low = jnp.where(former, rests[h], 0.0)
                carry[i * GROUP + 2 * j + h] = jnp.concatenate([top, low], axis=0).astype(jnp.bfloat16)
            if aims:
                base = thirds(all_rows(1.0 - norm))
                base = jnp.where(comp == 0, base[0], jnp.where(comp == 1, base[1], base[2]))
                aim = (
                    jnp.where(weigh, 1.0, 2.0 * one),
                    jnp.where(weigh, 0.0, 2.0 * two),
                    jnp.where(weigh, 0.0, 2.0 * three),
                    jnp.where(weigh, 0.0, base),
                )
                aim = [halves(part) for part in aim]
                for h in range(2):
                    a, b, c, d = [part[h] for part in aim]
                    narrow[i * GROUP + 2 * j + h] = jnp.concatenate(
                        [a, a, b, a, c, b, d, zeros], axis=0
                    ).astype(jnp.bfloat16)
        block = jnp.concatenate(tiles, axis=0).T.astype(jnp.bfloat16)
        for g in range(GROUP):
            pool[i * GROUP + g] = block * keep[g]

    def leaf_sums(leaf, out, where):
        near = [lists[e, leaf] for e in range(entries)]
        target = jnp.concatenate([narrow[leaf]] * 2, axis=0)
        pair = jnp.concatenate(
            [
                jnp.concatenate([target, blank], axis=1),
                jnp.concatenate([blank, target], axis=1),
            ],
            axis=0,
        )
        total = None
        for j in range(0, entries, 2):
            source = jnp.concatenate([pool[near[j]], pool[near[j + 1]]], axis=1)
            inside = jnp.dot(source, pair, preferred_element_type=jnp.float32)
            parts = []
            for half in range(2):
                close = inside[:, half * lanes : (half + 1) * lanes]
                inverse = lax.rsqrt((1.0 + soften_sq / cutoff_sq) - close)
                taper = jnp.maximum(close * inverse, 0.0)
                weight = taper * taper * inverse
                high = weight.astype(jnp.bfloat16)
                low = (weight - high.astype(jnp.float32)).astype(jnp.bfloat16)
                parts.append(jnp.concatenate([high, low], axis=1))
            moments = jnp.concatenate([carry[near[j]], carry[near[j + 1]]], axis=1)
            part = jnp.dot(
                moments, jnp.concatenate(parts, axis=0), preferred_element_type=jnp.float32
            )
            total = part if total is None else total + part
        out[rows_of(where, SUM_ROWS), :] = total[:, :lanes] + total[:, lanes:]

    def pull_of(out, first, second, place):
        sides = []
        for where in (first, second):
            both = out[rows_of(where * 2, PAIR), :] + out[rows_of(where * 2 + 1, PAIR), :]
            sides.append(both + roll(both, COMPS))
        moment = jnp.where(former, sides[0], sides[1])
        return moment - all_rows(moment) * place

    def lay_own(i, _):
        lay_group(i, [p[rows_of(2 * i + j, PAIR), :] for j in range(2)], True)
        return _

    def lay_lent(ref, at):
        for i in range(lent // GROUP):
            lay_group(
                leaves // GROUP + at * (lent // GROUP) + i,
                [ref[rows_of(2 * i + j, PAIR), :] for j in range(2)],
                False,
            )

    def pull(i, _):
        for u in range(UNROLL):
            leaf_sums(i * UNROLL + u, sums, i * UNROLL + u)
        return _

    def subcycle(k, lend):
        lax.fori_loop(0, leaves // GROUP, lay_own, 0, unroll=8)
        lay_lent(sent.at[k], slot_of(0, 0))
        for copy in copies(k):
            copy.wait_recv()
        for a, b in BESIDE:
            lay_lent(got.at[k, slot_of(a, b)], slot_of(a, b))
        if lend:
            for g in range(lent):
                leaf_sums(ghosts[g], ghost_sums, g)
            for g in range(0, lent, 2):
                rows = pl.ds(g * COMPS, PAIR)
                place = sent[k, rows, :]
                speed = ghost_v[rows, :] + moving * (
                    pull_of(ghost_sums, g, g + 1, place) + ghost_kick[rows, :]
                )
                ghost_v[rows, :] = speed
                sent[k + 1, rows, :] = place + moving * speed
            for copy in copies(k + 1):
                copy.start()
        lax.fori_loop(0, leaves // UNROLL, pull, 0)
        for leaf in range(0, leaves, 2):
            rows = pl.ds(leaf * COMPS, PAIR)
            place = p[rows, :]
            live = jnp.where(leaf + row // COMPS < count[0], moving, 0.0)
            speed = v[rows, :] + live * (pull_of(sums, leaf, leaf + 1, place) + kick[rows, :])
            v[rows, :] = speed
            p[rows, :] = place + live * speed

    def early(k, _):
        subcycle(k, True)
        return _

    lax.fori_loop(0, SUBCYCLES - 1, early, 0)
    subcycle(SUBCYCLES - 1, False)

    for leaf in range(leaves):
        at = pl.ds(leaf * COMPS, 3)
        p_out[leaf] = p[at, :]
        v_out[leaf] = v[at, :]

    for k in range(SUBCYCLES):
        for copy in copies(k):
            copy.wait_send()


def solution(mesh):
    sizes = (mesh.shape["gx"], mesh.shape["gy"])

    def body(positions, velocities, masses, long_kick, leaf_lists, ghost_ids, leaf_counts):
        leaves = leaf_lists.shape[1]
        lanes = masses.shape[0] // leaves
        lent = ghost_ids.shape[0]
        slots = leaves + len(WAYS) * lent
        state = jax.ShapeDtypeStruct((leaves, 3, lanes), jnp.float32)
        vmem = pl.BlockSpec(memory_space=pltpu.VMEM)
        smem = pl.BlockSpec(memory_space=pltpu.SMEM)
        f32 = jnp.float32

        def by_leaf(array):
            return array.reshape(3, leaves, lanes).transpose(1, 0, 2)

        places, speeds = pl.pallas_call(
            functools.partial(kernel, sizes),
            out_shape=(state, state),
            in_specs=[vmem] * 4 + [smem] * 3,
            out_specs=(vmem, vmem),
            scratch_shapes=[
                pltpu.VMEM((leaves * COMPS, lanes), f32),
                pltpu.VMEM((leaves * COMPS, lanes), f32),
                pltpu.VMEM((leaves * COMPS, lanes), f32),
                pltpu.VMEM((slots, lanes, lanes), jnp.bfloat16),
                pltpu.VMEM((slots, SUM_ROWS, lanes), jnp.bfloat16),
                pltpu.VMEM((leaves, TARGET_ROWS, lanes), jnp.bfloat16),
                pltpu.VMEM((leaves * SUM_ROWS, lanes), f32),
                pltpu.VMEM((lent * SUM_ROWS, lanes), f32),
                pltpu.VMEM((lent * COMPS, lanes), f32),
                pltpu.VMEM((lent * COMPS, lanes), f32),
                pltpu.VMEM((SUBCYCLES, lent * COMPS, lanes), f32),
                pltpu.VMEM((SUBCYCLES, len(WAYS), lent * COMPS, lanes), f32),
                pltpu.SemaphoreType.DMA((SUBCYCLES, len(WAYS))),
                pltpu.SemaphoreType.DMA((SUBCYCLES, len(WAYS))),
            ],
            compiler_params=pltpu.CompilerParams(collective_id=0, has_side_effects=True),
        )(
            by_leaf(positions),
            by_leaf(velocities),
            masses.reshape(leaves, lanes),
            by_leaf(long_kick),
            leaf_lists,
            ghost_ids,
            leaf_counts,
        )

        def by_part(array):
            return array.transpose(1, 0, 2).reshape(3, leaves * lanes)

        return by_part(places), by_part(speeds)

    return jax.shard_map(
        body,
        mesh=mesh,
        in_specs=(
            P(None, ("gx", "gy")),
            P(None, ("gx", "gy")),
            P(("gx", "gy")),
            P(None, ("gx", "gy")),
            P(None, ("gx", "gy")),
            P(("gx", "gy")),
            P(("gx", "gy")),
        ),
        out_specs=(P(None, ("gx", "gy")), P(None, ("gx", "gy"))),
        check_vma=False,
    )
```

```python
import functools

import jax
import jax.numpy as jnp
from jax import lax
from jax.experimental import pallas as pl
from jax.experimental.pallas import tpu as pltpu
from jax.sharding import PartitionSpec as P

SUBCYCLES = 4

soften_sq = 0.04
cutoff_sq = 9.0
time_step = 0.5

MESH = pl.DeviceIdType.MESH
COMPS = 4
PAIR = 2 * COMPS
GROUP = 4
SUM_ROWS = 16
TARGET_ROWS = 8 * PAIR
ROUND_UP = 1.0 + 2.0**-22
WAYS = [(a, b) for a in (-1, 0, 1) for b in (-1, 0, 1)]
BESIDE = [way for way in WAYS if way != (0, 0)]


def thirds(value):
    first = value.astype(jnp.bfloat16).astype(jnp.float32)
    rest = value - first
    second = rest.astype(jnp.bfloat16).astype(jnp.float32)
    return first, second, rest - second


def slot_of(a, b):
    return (a + 1) * 3 + b + 1


def kernel(
    sizes, p_in, v_in, mass, kick_in, lists, ghosts, count, p_out, v_out,
    p, v, kick, pool, carry, narrow, sums, ghost_v, ghost_kick, sent, got,
    send_sem, recv_sem,
):
    nx, ny = sizes
    leaves, lanes = mass.shape
    entries = lists.shape[0]
    lent = ghosts.shape[0]
    me_x, me_y = lax.axis_index("gx"), lax.axis_index("gy")

    def device(a, b):
        return (lax.rem(me_x + (a + nx), nx), lax.rem(me_y + (b + ny), ny))

    barrier = pltpu.get_barrier_semaphore()
    for a, b in BESIDE:
        pl.semaphore_signal(barrier, inc=1, device_id=device(a, b), device_id_type=MESH)

    def rows_of(index, height):
        return pl.ds(pl.multiple_of(index * height, height), height)

    for g in range(lent):
        leaf = ghosts[g]
        at = pl.ds(g * COMPS, 3)
        last = pl.ds(g * COMPS + 3, 1)
        sent[0, at, :] = p_in[leaf]
        sent[0, last, :] = mass[pl.ds(leaf, 1), :]
        ghost_v[at, :] = v_in[leaf]
        ghost_v[last, :] = jnp.zeros((1, lanes), jnp.float32)
        ghost_kick[at, :] = kick_in[leaf]
        ghost_kick[last, :] = jnp.zeros((1, lanes), jnp.float32)

    def copies(k):
        made = []
        for a, b in BESIDE:
            made.append(
                pltpu.make_async_remote_copy(
                    src_ref=sent.at[k],
                    dst_ref=got.at[k, slot_of(-a, -b)],
                    send_sem=send_sem.at[k, slot_of(a, b)],
                    recv_sem=recv_sem.at[k, slot_of(-a, -b)],
                    device_id=device(a, b),
                    device_id_type=MESH,
                )
            )
        return made

    pl.semaphore_wait(barrier, len(BESIDE))
    for copy in copies(0):
        copy.start()

    def flag(truth):
        return truth.astype(jnp.int32)

    ids = [ghosts[g] for g in range(lent)]
    new = []
    for g in range(lent):
        found = jnp.int32(1)
        for h in range(g):
            found = found * (1 - flag(ids[h] == ids[g]))
        new.append(found)
    total = sum(new)
    place_lent = [sum(new[h] * flag(ids[h] < ids[g]) for h in range(lent)) for g in range(lent)]
    order, place_of = [], []
    for s in range(leaves):
        leaf = s - total
        for g in range(lent):
            leaf = leaf + new[g] * flag(ids[g] - place_lent[g] <= s - total)
        if s < lent:
            for g in range(lent):
                leaf = leaf + new[g] * flag(place_lent[g] == s) * (ids[g] - leaf)
        order.append(leaf)
        place = total + s
        for g in range(lent):
            place = place - new[g] * flag(ids[g] < s)
        for g in range(lent):
            place = place + new[g] * flag(ids[g] == s) * (place_lent[g] - place)
        place_of.append(place)

    for leaf in range(leaves):
        at = pl.ds(leaf * COMPS, 3)
        last = pl.ds(leaf * COMPS + 3, 1)
        p[at, :] = p_in[leaf]
        p[last, :] = mass[pl.ds(leaf, 1), :]
        v[at, :] = v_in[leaf]
        v[last, :] = jnp.zeros((1, lanes), jnp.float32)
        kick[at, :] = kick_in[leaf]
        kick[last, :] = jnp.zeros((1, lanes), jnp.float32)

    row = lax.broadcasted_iota(jnp.int32, (PAIR, lanes), 0)
    comp = row % COMPS
    former = row < COMPS
    weigh = comp == COMPS - 1
    zeros = jnp.zeros((PAIR, lanes), jnp.float32)
    ones = jnp.ones((PAIR, lanes), jnp.float32)
    lane = lax.broadcasted_iota(jnp.int32, (lanes, lanes), 1)
    quarter = lane // TARGET_ROWS * 2 + lane % PAIR // COMPS
    keep = [(quarter == g).astype(jnp.float32).astype(jnp.bfloat16) for g in range(GROUP)]
    blank = jnp.zeros((lanes, lanes), jnp.bfloat16)
    moving = jnp.where(weigh, 0.0, time_step)

    def roll(value, by):
        return pltpu.roll(value, by, 0)

    def all_rows(value):
        filled = jnp.where(comp == 0, roll(value, PAIR - 3), value)
        filled = jnp.where(comp == 1, roll(value, PAIR - 2), filled)
        return jnp.where(comp == 2, roll(value, PAIR - 1), filled)

    def halves(value):
        swapped = roll(value, COMPS)
        return jnp.where(former, value, swapped), jnp.where(former, swapped, value)

    def spread(place):
        scaled = place * (cutoff_sq**-0.5)
        square = scaled * scaled
        norm = (roll(square, 1) + (roll(square, 2) + roll(square, 3))) * ROUND_UP
        return thirds(jnp.where(weigh, -norm, scaled)), norm

    def lay_group(i, places, aims):
        tiles = []
        for j, place in enumerate(places):
            (one, two, three), norm = spread(place)
            tiles += [one, two, one, three, one, two, ones, zeros]
            heavy = all_rows(place) * (cutoff_sq**-1.5)
            moments = thirds(heavy * jnp.where(weigh, 1.0, place))
            firsts, seconds, rests = [halves(moment) for moment in moments]
            for h in range(2):
                top = jnp.where(former, firsts[h], seconds[h])
                low = jnp.where(former, rests[h], 0.0)
                carry[i * GROUP + 2 * j + h] = jnp.concatenate([top, low], axis=0).astype(jnp.bfloat16)
            if aims:
                base = thirds(all_rows(1.0 - norm))
                base = jnp.where(comp == 0, base[0], jnp.where(comp == 1, base[1], base[2]))
                aim = (
                    jnp.where(weigh, 1.0, 2.0 * one),
                    jnp.where(weigh, 0.0, 2.0 * two),
                    jnp.where(weigh, 0.0, 2.0 * three),
                    jnp.where(weigh, 0.0, base),
                )
                aim = [halves(part) for part in aim]
                for h in range(2):
                    a, b, c, d = [part[h] for part in aim]
                    narrow[i * GROUP + 2 * j + h] = jnp.concatenate(
                        [a, a, b, a, c, b, d, zeros], axis=0
                    ).astype(jnp.bfloat16)
        block = jnp.concatenate(tiles, axis=0).T.astype(jnp.bfloat16)
        for g in range(GROUP):
            pool[i * GROUP + g] = block * keep[g]

    def leaf_sums(leaf, out, where):
        near = [lists[e, leaf] for e in range(entries)]
        target = jnp.concatenate([narrow[leaf]] * 2, axis=0)
        pair = jnp.concatenate(
            [
                jnp.concatenate([target, blank], axis=1),
                jnp.concatenate([blank, target], axis=1),
            ],
            axis=0,
        )
        total = None
        for j in range(0, entries, 2):
            source = jnp.concatenate([pool[near[j]], pool[near[j + 1]]], axis=1)
            inside = jnp.dot(source, pair, preferred_element_type=jnp.float32)
            parts = []
            for half in range(2):
                close = inside[:, half * lanes : (half + 1) * lanes]
                inverse = lax.rsqrt((1.0 + soften_sq / cutoff_sq) - close)
                taper = jnp.maximum(close * inverse, 0.0)
                weight = taper * taper * inverse
                high = weight.astype(jnp.bfloat16)
                low = (weight - high.astype(jnp.float32)).astype(jnp.bfloat16)
                parts.append(jnp.concatenate([high, low], axis=1))
            moments = jnp.concatenate([carry[near[j]], carry[near[j + 1]]], axis=1)
            part = jnp.dot(
                moments, jnp.concatenate(parts, axis=0), preferred_element_type=jnp.float32
            )
            total = part if total is None else total + part
        out[where] = total[:, :lanes] + total[:, lanes:]

    def pull_of(out, first, second, place):
        sides = []
        for where in (first, second):
            tile = out[where]
            both = tile[:PAIR] + tile[PAIR:]
            sides.append(both + roll(both, COMPS))
        moment = jnp.where(former, sides[0], sides[1])
        return moment - all_rows(moment) * place

    def lay_own(i, _):
        lay_group(i, [p[rows_of(2 * i + j, PAIR), :] for j in range(2)], True)
        return _

    def lay_lent(ref, at):
        for i in range(lent // GROUP):
            lay_group(
                leaves // GROUP + at * (lent // GROUP) + i,
                [ref[rows_of(2 * i + j, PAIR), :] for j in range(2)],
                False,
            )

    def pull(slots):
        for s in slots:
            leaf_sums(order[s], sums, s)

    def subcycle(k, carried):
        lax.fori_loop(0, leaves // GROUP, lay_own, 0, unroll=8)
        lay_lent(sent.at[k], slot_of(0, 0))
        for copy in copies(k):
            copy.wait_recv()
        for a, b in BESIDE:
            lay_lent(got.at[k, slot_of(a, b)], slot_of(a, b))
        pull(range(lent))
        for g in range(0, lent, 2):
            rows = pl.ds(g * COMPS, PAIR)
            place = sent[k, rows, :]
            speed = ghost_v[rows, :] + moving * (
                pull_of(sums, place_lent[g], place_lent[g + 1], place) + ghost_kick[rows, :]
            )
            ghost_v[rows, :] = speed
            sent[k + 1, rows, :] = place + moving * speed
        for copy in copies(k + 1):
            copy.start()
        pull(range(lent, leaves))
        for leaf in range(0, leaves, 2):
            rows = pl.ds(leaf * COMPS, PAIR)
            place = p[rows, :]
            live = jnp.where(leaf + row // COMPS < count[0], moving, 0.0)
            accel = pull_of(sums, place_of[leaf], place_of[leaf + 1], place)
            speed = v[rows, :] + live * (accel + kick[rows, :])
            v[rows, :] = speed
            p[rows, :] = place + live * speed
        return carried

    lax.fori_loop(0, SUBCYCLES, subcycle, 0)

    for leaf in range(leaves):
        at = pl.ds(leaf * COMPS, 3)
        p_out[leaf] = p[at, :]
        v_out[leaf] = v[at, :]

    for copy in copies(SUBCYCLES):
        copy.wait_recv()
    for k in range(SUBCYCLES + 1):
        for copy in copies(k):
            copy.wait_send()


def solution(mesh):
    sizes = (mesh.shape["gx"], mesh.shape["gy"])

    def body(positions, velocities, masses, long_kick, leaf_lists, ghost_ids, leaf_counts):
        leaves = leaf_lists.shape[1]
        lanes = masses.shape[0] // leaves
        lent = ghost_ids.shape[0]
        slots = leaves + len(WAYS) * lent
        state = jax.ShapeDtypeStruct((leaves, 3, lanes), jnp.float32)
        vmem = pl.BlockSpec(memory_space=pltpu.VMEM)
        smem = pl.BlockSpec(memory_space=pltpu.SMEM)
        f32 = jnp.float32

        def by_leaf(array):
            return array.reshape(3, leaves, lanes).transpose(1, 0, 2)

        places, speeds = pl.pallas_call(
            functools.partial(kernel, sizes),
            out_shape=(state, state),
            in_specs=[vmem] * 4 + [smem] * 3,
            out_specs=(vmem, vmem),
            scratch_shapes=[
                pltpu.VMEM((leaves * COMPS, lanes), f32),
                pltpu.VMEM((leaves * COMPS, lanes), f32),
                pltpu.VMEM((leaves * COMPS, lanes), f32),
                pltpu.VMEM((slots, lanes, lanes), jnp.bfloat16),
                pltpu.VMEM((slots, SUM_ROWS, lanes), jnp.bfloat16),
                pltpu.VMEM((leaves, TARGET_ROWS, lanes), jnp.bfloat16),
                pltpu.VMEM((leaves, SUM_ROWS, lanes), f32),
                pltpu.VMEM((lent * COMPS, lanes), f32),
                pltpu.VMEM((lent * COMPS, lanes), f32),
                pltpu.VMEM((SUBCYCLES + 1, lent * COMPS, lanes), f32),
                pltpu.VMEM((SUBCYCLES + 1, len(WAYS), lent * COMPS, lanes), f32),
                pltpu.SemaphoreType.DMA((SUBCYCLES + 1, len(WAYS))),
                pltpu.SemaphoreType.DMA((SUBCYCLES + 1, len(WAYS))),
            ],
            compiler_params=pltpu.CompilerParams(collective_id=0, has_side_effects=True),
        )(
            by_leaf(positions),
            by_leaf(velocities),
            masses.reshape(leaves, lanes),
            by_leaf(long_kick),
            leaf_lists,
            ghost_ids,
            leaf_counts,
        )

        def by_part(array):
            return array.transpose(1, 0, 2).reshape(3, leaves * lanes)

        return by_part(places), by_part(speeds)

    return jax.shard_map(
        body,
        mesh=mesh,
        in_specs=(
            P(None, ("gx", "gy")),
            P(None, ("gx", "gy")),
            P(("gx", "gy")),
            P(None, ("gx", "gy")),
            P(None, ("gx", "gy")),
            P(("gx", "gy")),
            P(("gx", "gy")),
        ),
        out_specs=(P(None, ("gx", "gy")), P(None, ("gx", "gy"))),
        check_vma=False,
    )
```
